256 devices in a mesh: tm: 128 (over y_hi, z, x, core), mom: 2 (over y_lo).
Axes of the slice: x: 4, y: 4 (y_hi: 2, y_lo: 2; y = y_hi * 2 + y_lo), z: 8, core: 2. Of those that a mesh axis runs over, the one named last changes fastest.
Arguments:
- fields: bfloat16 [128, 4, 2, 512, 512], P('tm', 'mom'), may hold values from -1 to 1
- mom_pairs: int32 [6, 2], P('mom'), may hold values from 0 to 3, as said below
- deltas: int32 [4], replicated, may hold values from 0 to 3, each once
Outputs:
- time_traces: float32 [128, 2, 4, 6], P('tm', None, None, 'mom')
- summed_traces: float32 [2, 4, 6], P(None, None, 'mom')
The draws below stay inside these ranges and needn't reach their ends.
Inputs may be any that keep to these rules, and one draw needn't show every extreme that they name: `mom_pairs`: column 0 may be any momentum; in row r, column 1 lies in momentum group r // 3, that is from (r // 3) * 2 to (r // 3) * 2 + 1.
All inputs are finite; a program needn't handle non-finite values.
Results may differ from the reference program's by a relative error of at most 0.0003.
Values may be sent and summed in bfloat16 or wider, within the bound.
No kernel may reach another device: no remote copies, remote signals or barrier semaphores. Data moves between devices by JAX's collectives and lax.ppermute only.
A program may use at most 128 MiB of HBM per device.

```python
import jax
import jax.numpy as jnp
from jax import lax

NEV = 512
PG = 2
PAIR_DEV = 3
NSEP = 4
P_SIZE = 4
NPAIR = 6
NT = 128


def draw_fields(key, part):
    field_shape = (NT, P_SIZE, 2, NEV, NEV)
    key_base = jax.random.fold_in(jax.random.fold_in(key, 11), 0)
    growth = jnp.sqrt(3.0) ** (jnp.arange(NT, dtype=jnp.float32) / max(NT - 1, 1))
    values = jax.random.normal(key_base, field_shape, jnp.float32)
    values = values * growth[:, None, None, None, None] / jnp.sqrt(jnp.float32(NEV))
    return jnp.clip(values, -1.0, 1.0).astype(jnp.bfloat16)


def draw_mom_pairs(key, part):
    key_source, key_target = jax.random.split(jax.random.fold_in(key, 23), 2)
    source_mom = jax.random.randint(key_source, (NPAIR,), 0, P_SIZE)
    owner = jnp.arange(NPAIR, dtype=jnp.int32) // PAIR_DEV
    target_mom = owner * PG + jax.random.randint(key_target, (NPAIR,), 0, PG)
    return jnp.stack([source_mom, target_mom], axis=1).astype(jnp.int32)


def setup_inputs(seed: int = 0) -> dict:
    streams_of = jax.random.split(jax.random.key(seed), 4)
    fields = draw_fields(jax.random.fold_in(streams_of[3], 71), 0)
    mom_pairs = draw_mom_pairs(jax.random.fold_in(streams_of[3], 71), 0)
    deltas = jax.random.permutation(streams_of[2], NSEP).astype(jnp.int32)
    return dict(fields=fields, mom_pairs=mom_pairs, deltas=deltas)


def products(source, target):
    product_full = jnp.einsum("xij,yjk->xyik", source.astype(jnp.float32), target.astype(jnp.float32))
    real_part = product_full[0, 0] - product_full[1, 1]
    imag_part = product_full[0, 1] + product_full[1, 0]
    direct = jnp.trace(real_part)
    box_value = jnp.sum(real_part * real_part.T) - jnp.sum(imag_part * imag_part.T)
    return direct, box_value


def reference(fields, mom_pairs, deltas):
    slices = fields.shape[0]
    pair_count = mom_pairs.shape[0]

    def one_time(time_slice):
        source_slice = lax.dynamic_index_in_dim(fields, time_slice, 0, keepdims=False)
        per_sep = []
        for separation in range(1, NSEP + 1):
            later = ((time_slice + separation) % slices).astype(jnp.int32)
            target_slice = lax.dynamic_index_in_dim(fields, later, 0, keepdims=False)
            directs = []
            boxes = []
            for which in range(pair_count):
                source = lax.dynamic_index_in_dim(source_slice, mom_pairs[which, 0].astype(jnp.int32), 0, keepdims=False)
                target = lax.dynamic_index_in_dim(target_slice, mom_pairs[which, 1].astype(jnp.int32), 0, keepdims=False)
                direct, box_value = products(source, target)
                directs.append(direct)
                boxes.append(box_value)
            per_sep.append(jnp.stack([jnp.stack(directs), jnp.stack(boxes)]))
        return jnp.stack(per_sep, axis=1)

    stacked = lax.map(one_time, jnp.arange(slices, dtype=jnp.int32))
    time_traces = jnp.take(stacked, deltas.astype(jnp.int32), axis=2)
    summed_traces = jnp.sum(time_traces, axis=0)
    return time_traces, summed_traces
```

```python
import jax
import jax.numpy as jnp
from jax import lax
from jax.experimental import pallas as pl
from jax.experimental.pallas import tpu as pltpu
from jax.sharding import Mesh
from jax.sharding import PartitionSpec as P

TM = ("tm_0", "tm_1", "tm_2", "tm_3")
ALL = TM + ("mom",)
SIZES = (2, 8, 4, 2, 2)
F32 = jnp.float32
BF16 = jnp.bfloat16
N = 512
TIMES = 128
HALF = 64
ROWS = 384


def place(time):
    rest, core = divmod(time, 2)
    rest, x = divmod(rest, 4)
    half, z = divmod(rest, 8)
    return half, z, x, core


def time_of(half, z, x, core):
    return ((half * 8 + z) * 4 + x) * 2 + core


def device(time, group):
    return time * 2 + group


def each():
    return ((time, group) for time in range(TIMES) for group in range(2))


def earlier(time, group, distance):
    target = (time - distance) % TIMES
    crossed = place(target)[0] != place(time)[0]
    return target, group ^ crossed


def ring_route(distance):
    return [(device(t, g), device(*earlier(t, g, distance))) for t, g in each()]


def round_x_holder(time, group):
    half, z, x, core = place(time)
    if x == 1:
        target, kept = earlier(time, group, 4)
        half, z, _, _ = place(target)
        return time_of(half, z, 2, core), kept
    return time_of(half, z, (x + 1) % 4, core), group


def round_x_first():
    return [(device(t, g), device(*round_x_holder(t, g))) for t, g in each()]


def round_x_second():
    return [(device(*round_x_holder(t, g)), device(*earlier(t, g, 4))) for t, g in each()]


def partner_group_route():
    return [(device(t, g), device(t, 1 - g)) for t, g in each()]


def other_core_route():
    return [(device(t, g), device(t ^ 1, g)) for t, g in each()]


def to_core(core):
    return [(device(t ^ 1, g), device(t, g)) for t, g in each() if t % 2 == core]


def of_core(route, core):
    return [(a, b) for a, b in route if (a // 2) % 2 == core]


def moved(array, route):
    return lax.ppermute(array, ALL, route)


TIME, GROUP, PAIRS, OTHER_PAIRS, DELTAS = 0, 1, 2, 8, 14
SMEM = pl.BlockSpec(memory_space=pltpu.SMEM)
VMEM = pl.BlockSpec(memory_space=pltpu.VMEM)
ANYWHERE = pl.BlockSpec(memory_space=pl.ANY)
HBM = pl.BlockSpec(memory_space=pltpu.HBM)


def fold(block):
    rows, columns = block.shape
    block = block.reshape(rows // 8, 8, columns).sum(0)
    return sum(block[:, i * 128 : (i + 1) * 128] for i in range(columns // 128))


def diagonal(block):
    rows = lax.broadcasted_iota(jnp.int32, block.shape, 0)
    columns = lax.broadcasted_iota(jnp.int32, block.shape, 1)
    return jnp.where(rows == columns, block, 0.0)


def product_terms(source, target, diff, total):
    direct = jnp.zeros((8, 128), F32)

    def dot(left, right):
        return jnp.dot(left, right, preferred_element_type=F32)

    for tile in range(2):
        columns = slice(tile * 256, (tile + 1) * 256)
        right_re = jnp.concatenate([piece[0, :, columns] for piece in target], axis=0)
        right_im = jnp.concatenate([piece[1, :, columns] for piece in target], axis=0)
        for half in range(2):
            rows = slice(half * 256, (half + 1) * 256)
            left_re, left_im = source[0, rows], source[1, rows]
            q_re = dot(left_re, right_re) - dot(left_im, right_im)
            q_im = dot(left_re, right_im) + dot(left_im, right_re)
            if half == tile:
                for k in range(2):
                    at = slice(k * 128, (k + 1) * 128)
                    direct = direct + fold(diagonal(q_re[at, at]))
            diff[rows, columns] = q_re - q_im
            total[rows, columns] = q_re + q_im
    box = jnp.zeros((8, 128), F32)
    for i in range(4):
        rows = slice(i * 128, (i + 1) * 128)
        for j in range(4):
            columns = slice(j * 128, (j + 1) * 128)
            box = box + fold(diff[rows, columns] * total[columns, rows].T)
    return direct, box


def add_terms(table, fields, result, sep, pieces, diff, total):
    time, group = table[TIME], table[GROUP]
    crossed = (time % HALF) + sep >= HALF
    shown = jnp.where(crossed, 1 - group, group)
    at = jnp.where(crossed, OTHER_PAIRS, PAIRS)
    row = sum(jnp.where(table[DELTAS + i] == sep - 1, i, 0) for i in range(4))
    lanes = lax.broadcasted_iota(jnp.int32, (1, 128), 1)
    for k in range(3):
        source = table[at + 2 * k]
        slot = source % 2 + jnp.where(source // 2 == group, 0, 2)
        momentum = table[at + 2 * k + 1] - 2 * shown

        target = [piece.at[momentum] for piece in pieces]
        direct, box = product_terms(fields.at[slot], target, diff.at[k % 2], total.at[k % 2])
        result = jnp.where(lanes == k * 4 + row, jnp.sum(direct), result)
        result = jnp.where(lanes == 12 + k * 4 + row, jnp.sum(box), result)
    return result


def first_body(
    table_in, own, other, near, two, out, fields, table, near_in, two_in, diff, total, sems
):
    moves = [
        (table_in, table),
        (own, fields.at[0:2]),
        (other, fields.at[2:4]),
        (near, near_in),
        (two, two_in),
    ]
    copies = [pltpu.make_async_copy(a, b, sems.at[i]) for i, (a, b) in enumerate(moves)]
    for copy in copies[:3]:
        copy.start()
    copies[0].wait()
    core = table[TIME] % 2
    pl.when(core == 0)(copies[3].start)
    copies[4].start()
    copies[1].wait()
    copies[2].wait()
    out[...] = jnp.zeros((1, 128), F32)

    @pl.when(core == 0)
    def _():
        copies[3].wait()
        out[...] = add_terms(table, fields, out[...], 1, [near_in], diff, total)

    copies[4].wait()
    out[...] = add_terms(table, fields, out[...], 2, [two_in], diff, total)


def swapped_body(table, fields, later, before, out, diff, total):
    sep = jnp.where(table[TIME] % 2 == 0, 3, 1)
    out[...] = add_terms(table, fields, before[...], sep, [later], diff, total)


def late_body(table, fields, later, before, out, diff, total):
    out[...] = before[...]

    @pl.when(table[TIME] % 2 == 1)
    def _():
        out[...] = add_terms(table, fields, before[...], 3, [later], diff, total)


def four_body(table, fields, around, onward, rest, before, out, around_in, diff, total, sems):
    core = table[TIME] % 2

    def put(*later):
        result = add_terms(table, fields, before[...], 4, later, diff, total)
        out[...] = jnp.broadcast_to(result[None], out.shape)

    @pl.when(core == 0)
    def _():
        copy = pltpu.make_async_copy(around, around_in, sems.at[0])
        copy.start()
        copy.wait()
        put(around_in)

    @pl.when(core == 1)
    def _():
        put(onward, rest)


ROW = jax.ShapeDtypeStruct((1, 128), F32)
FIELDS = jax.ShapeDtypeStruct((4, 2, N, N), BF16)
PLANES = pltpu.VMEM((2, 2, N, N), BF16)
WORK = [pltpu.VMEM((2, N, N), F32), pltpu.VMEM((2, N, N), F32)]


def stage(body, operands, spaces, outs, scratch, products):
    call = pl.pallas_call(
        body,
        in_specs=spaces,
        out_specs=jax.tree.map(lambda _: VMEM, outs),
        out_shape=outs,
        scratch_shapes=scratch,
        compiler_params=pltpu.CompilerParams(vmem_limit_bytes=20 << 20),
        cost_estimate=pl.CostEstimate(
            flops=products * 8 * N**3, bytes_accessed=5 << 20, transcendentals=0
        ),
    )
    return call(*operands)


def zero_body(table, out):
    out[...] = jnp.zeros((1, 128), F32)


def mark_body(before, _, out):
    out[...] = before[...]


def finish_body(table, gathered, _, time_out, sum_out, time_row, sum_row, sems):
    time, group = table[TIME], table[GROUP]
    lanes = lax.broadcasted_iota(jnp.int32, (1, 128), 1)
    sep = jnp.zeros((1, 128), jnp.int32)
    for r in range(4):
        sep = jnp.where(lanes % 4 == r, table[DELTAS + r] + 1, sep)

    def value(at):
        crossed = (at % HALF) + sep >= HALF
        return jnp.where(crossed, gathered[2 * at + 1 - group], gathered[2 * at + group])

    def spread(row, out):
        for val in range(2):
            for k in range(3):
                at = val * 12 + k * 4
                shifted = pltpu.roll(row, 128 - at, 1) if at else row
                out[k, val : val + 1, :] = shifted[:, 0:4]

    spread(value(time), time_row.at[0])
    mine = pltpu.make_async_copy(time_row, time_out, sems.at[0])
    mine.start()
    total = jnp.zeros((1, 128), F32)
    for at in range(TIMES):
        if at % HALF < HALF - 4:
            total = total + gathered[2 * at + group]
        else:
            total = total + value(at)
    spread(total, sum_row)
    both = pltpu.make_async_copy(sum_row, sum_out, sems.at[1])
    both.start()
    mine.wait()
    both.wait()


def finished(table, gathered, ready):
    shapes = ((1, 3, 2, 4), (3, 2, 4))
    call = pl.pallas_call(
        finish_body,
        in_specs=[SMEM, VMEM, ANYWHERE],
        out_specs=(HBM, HBM),
        out_shape=tuple(jax.ShapeDtypeStruct(shape, F32) for shape in shapes),
        scratch_shapes=[pltpu.VMEM(shape, F32) for shape in shapes]
        + [pltpu.SemaphoreType.DMA((2,))],
        name="finish",
    )
    time_traces, summed_traces = call(table, gathered, ready)
    return time_traces.transpose(0, 2, 3, 1), summed_traces.transpose(1, 2, 0)


def per_device(fields, mom_pairs, deltas):
    own = fields[0]
    time = lax.axis_index(TM).astype(jnp.int32)
    group = lax.axis_index("mom").astype(jnp.int32)

    two = moved(own, ring_route(2))
    other_pairs = moved(mom_pairs, partner_group_route())
    other = moved(own, partner_group_route())
    around = moved(own, of_core(round_x_first(), 0))
    near = moved(own, to_core(0))
    table = jnp.concatenate(
        [jnp.stack([time, group]), mom_pairs.reshape(-1), other_pairs.reshape(-1), deltas]
    )
    zero = pl.pallas_call(zero_body, in_specs=[SMEM], out_specs=VMEM, out_shape=ROW, name="zero")
    mark = pl.pallas_call(
        mark_body, in_specs=[VMEM, VMEM], out_specs=VMEM, out_shape=ROW, name="mark"
    )
    ready = mark(zero(table), own)
    around = moved(around, of_core(round_x_second(), 0))
    swap = moved(two, other_core_route())
    onward = moved(two[:, :, :ROWS], of_core(ring_route(2), 1))
    rest = moved(own[:, :, ROWS:], of_core(round_x_first(), 1))
    rest = moved(rest, of_core(round_x_second(), 1))

    result, all_fields = stage(
        first_body,
        (table, own, other, near, two),
        [HBM, VMEM] + [ANYWHERE] * 3,
        (ROW, FIELDS),
        [pltpu.SMEM((18,), jnp.int32), PLANES, PLANES] + WORK + [pltpu.SemaphoreType.DMA((5,))],
        6,
    )
    late = moved(around, to_core(1))
    result = stage(
        swapped_body, (table, all_fields, swap, result), [SMEM] + [VMEM] * 3, ROW, WORK, 3
    )
    result = stage(late_body, (table, all_fields, late, result), [SMEM] + [VMEM] * 3, ROW, WORK, 3)
    rows = stage(
        four_body,
        (table, all_fields, around, onward, rest, result),
        [SMEM, VMEM, ANYWHERE, VMEM, VMEM, VMEM],
        jax.ShapeDtypeStruct((2 * TIMES, 1, 128), F32),
        [PLANES] + WORK + [pltpu.SemaphoreType.DMA((1,))],
        3,
    )
    gathered = lax.all_to_all(rows, ALL, 0, 0, tiled=True)
    return finished(table, gathered, ready)


def solution(mesh):
    finer = Mesh(mesh.devices.reshape(SIZES), ALL)
    in_specs = (P(TM, "mom", None, None, None), P("mom", None), P())
    out_specs = (P(TM, None, None, "mom"), P(None, None, "mom"))
    return jax.shard_map(
        per_device, mesh=finer, in_specs=in_specs, out_specs=out_specs, check_vma=False
    )
```

```python
import functools

import jax
import jax.numpy as jnp
from jax import lax
from jax.experimental import pallas as pl
from jax.experimental.pallas import tpu as pltpu
from jax.sharding import Mesh
from jax.sharding import PartitionSpec as P

TM = ("tm_0", "tm_1", "tm_2", "tm_3")
ALL = TM + ("mom",)
SIZES = (2, 8, 4, 2, 2)
F32 = jnp.float32
BF16 = jnp.bfloat16
N = 512
TIMES = 128
HALF = 64
ROWS = 416


def place(time):
    rest, core = divmod(time, 2)
    rest, x = divmod(rest, 4)
    half, z = divmod(rest, 8)
    return half, z, x, core


def time_of(half, z, x, core):
    return ((half * 8 + z) * 4 + x) * 2 + core


def device(time, group):
    return time * 2 + group


def each():
    return ((time, group) for time in range(TIMES) for group in range(2))


def earlier(time, group, distance):
    target = (time - distance) % TIMES
    crossed = place(target)[0] != place(time)[0]
    return target, group ^ crossed


def ring_route(distance):
    return [(device(t, g), device(*earlier(t, g, distance))) for t, g in each()]


def round_x_holder(time, group):
    half, z, x, core = place(time)
    if x == 1:
        target, kept = earlier(time, group, 4)
        half, z, _, _ = place(target)
        return time_of(half, z, 2, core), kept
    return time_of(half, z, (x + 1) % 4, core), group


def round_x_first():
    return [(device(t, g), device(*round_x_holder(t, g))) for t, g in each()]


def round_x_second():
    return [(device(*round_x_holder(t, g)), device(*earlier(t, g, 4))) for t, g in each()]


def partner_group_route():
    return [(device(t, g), device(t, 1 - g)) for t, g in each()]


def to_core(core):
    return [(device(t ^ 1, g), device(t, g)) for t, g in each() if t % 2 == core]


def of_core(route, core):
    return [(a, b) for a, b in route if (a // 2) % 2 == core]


def moved(array, route):
    return lax.ppermute(array, ALL, route)


TIME, GROUP, PAIRS, OTHER_PAIRS, DELTAS = 0, 1, 2, 8, 14
SMEM = pl.BlockSpec(memory_space=pltpu.SMEM)
VMEM = pl.BlockSpec(memory_space=pltpu.VMEM)
ANYWHERE = pl.BlockSpec(memory_space=pl.ANY)
HBM = pl.BlockSpec(memory_space=pltpu.HBM)


def fold(block):
    rows, columns = block.shape
    block = block.reshape(rows // 8, 8, columns).sum(0)
    return sum(block[:, i * 128 : (i + 1) * 128] for i in range(columns // 128))


def diagonal(block):
    rows = lax.broadcasted_iota(jnp.int32, block.shape, 0)
    columns = lax.broadcasted_iota(jnp.int32, block.shape, 1)
    return jnp.where(rows == columns, block, 0.0)


def product_terms(source, target, diff, total):
    direct = jnp.zeros((8, 128), F32)

    def dot(left, right):
        return jnp.dot(left, right, preferred_element_type=F32)

    for tile in range(2):
        columns = slice(tile * 256, (tile + 1) * 256)
        right_re = jnp.concatenate([piece[0, :, columns] for piece in target], axis=0)
        right_im = jnp.concatenate([piece[1, :, columns] for piece in target], axis=0)
        for half in range(2):
            rows = slice(half * 256, (half + 1) * 256)
            left_re, left_im = source[0, rows], source[1, rows]
            q_re = dot(left_re, right_re) - dot(left_im, right_im)
            q_im = dot(left_re, right_im) + dot(left_im, right_re)
            if half == tile:
                for k in range(2):
                    at = slice(k * 128, (k + 1) * 128)
                    direct = direct + fold(diagonal(q_re[at, at]))
            diff[rows, columns] = q_re - q_im
            total[rows, columns] = q_re + q_im
    box = jnp.zeros((8, 128), F32)
    for i in range(4):
        rows = slice(i * 128, (i + 1) * 128)
        for j in range(4):
            columns = slice(j * 128, (j + 1) * 128)
            box = box + fold(diff[rows, columns] * total[columns, rows].T)
    return direct, box


def add_terms(table, fields, result, sep, pieces, diff, total):
    time, group = table[TIME], table[GROUP]
    crossed = (time % HALF) + sep >= HALF
    shown = jnp.where(crossed, 1 - group, group)
    at = jnp.where(crossed, OTHER_PAIRS, PAIRS)
    row = sum(jnp.where(table[DELTAS + i] == sep - 1, i, 0) for i in range(4))
    lanes = lax.broadcasted_iota(jnp.int32, (1, 128), 1)
    for k in range(3):
        source = table[at + 2 * k]
        slot = source % 2 + jnp.where(source // 2 == group, 0, 2)
        momentum = table[at + 2 * k + 1] - 2 * shown

        target = [piece.at[momentum] for piece in pieces]
        direct, box = product_terms(fields.at[slot], target, diff.at[k % 2], total.at[k % 2])
        result = jnp.where(lanes == k * 4 + row, jnp.sum(direct), result)
        result = jnp.where(lanes == 12 + k * 4 + row, jnp.sum(box), result)
    return result


def first_body(table_in, own, other, near, out, fields, table, near_in, diff, total, sems):
    moves = [(table_in, table), (own, fields.at[0:2]), (other, fields.at[2:4]), (near, near_in)]
    copies = [pltpu.make_async_copy(a, b, sems.at[i]) for i, (a, b) in enumerate(moves)]
    for copy in copies[:3]:
        copy.start()
    copies[0].wait()
    core = table[TIME] % 2
    pl.when(core == 0)(copies[3].start)
    copies[1].wait()
    copies[2].wait()
    out[...] = jnp.zeros((1, 128), F32)

    @pl.when(core == 0)
    def _():
        copies[3].wait()
        out[...] = add_terms(table, fields, out[...], 1, [near_in], diff, total)


def by_core_body(table, fields, later0, later1, before, out, diff, total, *, seps):
    for core, later in enumerate((later0, later1)):

        @pl.when(table[TIME] % 2 == core)
        def _(core=core, later=later):
            out[...] = add_terms(
                table, fields, before[...], seps[core], [later], diff, total
            )


def late_body(table, fields, later, before, out, diff, total):
    out[...] = before[...]

    @pl.when(table[TIME] % 2 == 1)
    def _():
        out[...] = add_terms(table, fields, before[...], 3, [later], diff, total)


def four_body(table, fields, around, onward, rest, before, out, around_in, diff, total, sems):
    core = table[TIME] % 2

    def put(*later):
        result = add_terms(table, fields, before[...], 4, later, diff, total)
        out[...] = jnp.broadcast_to(result[None], out.shape)

    @pl.when(core == 0)
    def _():
        copy = pltpu.make_async_copy(around, around_in, sems.at[0])
        copy.start()
        copy.wait()
        put(around_in)

    @pl.when(core == 1)
    def _():
        put(onward, rest)


ROW = jax.ShapeDtypeStruct((1, 128), F32)
FIELDS = jax.ShapeDtypeStruct((4, 2, N, N), BF16)
PLANES = pltpu.VMEM((2, 2, N, N), BF16)
WORK = [pltpu.VMEM((2, N, N), F32), pltpu.VMEM((2, N, N), F32)]


def stage(body, operands, spaces, outs, scratch, products):
    call = pl.pallas_call(
        body,
        in_specs=spaces,
        out_specs=jax.tree.map(lambda _: VMEM, outs),
        out_shape=outs,
        scratch_shapes=scratch,
        compiler_params=pltpu.CompilerParams(vmem_limit_bytes=20 << 20),
        cost_estimate=pl.CostEstimate(
            flops=products * 8 * N**3, bytes_accessed=5 << 20, transcendentals=0
        ),
    )
    return call(*operands)


def zero_body(table, out):
    out[...] = jnp.zeros((1, 128), F32)


def mark_body(before, _, out):
    out[...] = before[...]


def finish_body(table, gathered, _, time_out, sum_out, time_row, sum_row, sems):
    time, group = table[TIME], table[GROUP]
    lanes = lax.broadcasted_iota(jnp.int32, (1, 128), 1)
    sep = jnp.zeros((1, 128), jnp.int32)
    for r in range(4):
        sep = jnp.where(lanes % 4 == r, table[DELTAS + r] + 1, sep)

    def value(at):
        crossed = (at % HALF) + sep >= HALF
        return jnp.where(crossed, gathered[2 * at + 1 - group], gathered[2 * at + group])

    def spread(row, out):
        for val in range(2):
            for k in range(3):
                at = val * 12 + k * 4
                shifted = pltpu.roll(row, 128 - at, 1) if at else row
                out[k, val : val + 1, :] = shifted[:, 0:4]

    spread(value(time), time_row.at[0])
    mine = pltpu.make_async_copy(time_row, time_out, sems.at[0])
    mine.start()
    total = jnp.zeros((1, 128), F32)
    for at in range(TIMES):
        if at % HALF < HALF - 4:
            total = total + gathered[2 * at + group]
        else:
            total = total + value(at)
    spread(total, sum_row)
    both = pltpu.make_async_copy(sum_row, sum_out, sems.at[1])
    both.start()
    mine.wait()
    both.wait()


def finished(table, gathered, ready):
    shapes = ((1, 3, 2, 4), (3, 2, 4))
    call = pl.pallas_call(
        finish_body,
        in_specs=[SMEM, VMEM, ANYWHERE],
        out_specs=(HBM, HBM),
        out_shape=tuple(jax.ShapeDtypeStruct(shape, F32) for shape in shapes),
        scratch_shapes=[pltpu.VMEM(shape, F32) for shape in shapes]
        + [pltpu.SemaphoreType.DMA((2,))],
        name="finish",
    )
    time_traces, summed_traces = call(table, gathered, ready)
    return time_traces.transpose(0, 2, 3, 1), summed_traces.transpose(1, 2, 0)


def per_device(fields, mom_pairs, deltas):
    own = fields[0]
    time = lax.axis_index(TM).astype(jnp.int32)
    group = lax.axis_index("mom").astype(jnp.int32)

    two1 = moved(own, of_core(ring_route(2), 1))
    other_pairs = moved(mom_pairs, partner_group_route())
    other = moved(own, partner_group_route())
    around = moved(own, of_core(round_x_first(), 0))
    near = moved(own, to_core(0))
    table = jnp.concatenate(
        [jnp.stack([time, group]), mom_pairs.reshape(-1), other_pairs.reshape(-1), deltas]
    )
    zero = pl.pallas_call(zero_body, in_specs=[SMEM], out_specs=VMEM, out_shape=ROW, name="zero")
    mark = pl.pallas_call(
        mark_body, in_specs=[VMEM, VMEM], out_specs=VMEM, out_shape=ROW, name="mark"
    )
    ready = mark(zero(table), own)
    around = moved(around, of_core(round_x_second(), 0))
    two0 = moved(own, of_core(ring_route(2), 0))
    onward = moved(two1[:, :, :ROWS], of_core(ring_route(2), 1))
    swap1 = moved(two1, to_core(0))
    swap0 = moved(two0, to_core(1))
    rest = moved(own[:, :, ROWS:], of_core(round_x_first(), 1))
    rest = moved(rest, of_core(round_x_second(), 1))

    result, all_fields = stage(
        first_body,
        (table, own, other, near),
        [HBM, VMEM] + [ANYWHERE] * 2,
        (ROW, FIELDS),
        [pltpu.SMEM((18,), jnp.int32), PLANES] + WORK + [pltpu.SemaphoreType.DMA((4,))],
        3,
    )
    result = stage(
        functools.partial(by_core_body, seps=(2, 2)),
        (table, all_fields, two0, two1, result),
        [SMEM] + [VMEM] * 4,
        ROW,
        WORK,
        3,
    )
    late = moved(around, to_core(1))
    result = stage(
        functools.partial(by_core_body, seps=(3, 1)),
        (table, all_fields, swap1, swap0, result),
        [SMEM] + [VMEM] * 4,
        ROW,
        WORK,
        3,
    )
    result = stage(late_body, (table, all_fields, late, result), [SMEM] + [VMEM] * 3, ROW, WORK, 3)
    rows = stage(
        four_body,
        (table, all_fields, around, onward, rest, result),
        [SMEM, VMEM, ANYWHERE, VMEM, VMEM, VMEM],
        jax.ShapeDtypeStruct((2 * TIMES, 1, 128), F32),
        [PLANES] + WORK + [pltpu.SemaphoreType.DMA((1,))],
        3,
    )
    gathered = lax.all_to_all(rows, ALL, 0, 0, tiled=True)
    return finished(table, gathered, ready)


def solution(mesh):
    finer = Mesh(mesh.devices.reshape(SIZES), ALL)
    in_specs = (P(TM, "mom", None, None, None), P("mom", None), P())
    out_specs = (P(TM, None, None, "mom"), P(None, None, "mom"))
    return jax.shard_map(
        per_device, mesh=finer, in_specs=in_specs, out_specs=out_specs, check_vma=False
    )
```

```python
import functools

import jax
import jax.numpy as jnp
from jax import lax
from jax.experimental import pallas as pl
from jax.experimental.pallas import tpu as pltpu
from jax.sharding import Mesh
from jax.sharding import PartitionSpec as P

TM = ("tm_0", "tm_1", "tm_2", "tm_3")
ALL = TM + ("mom",)
SIZES = (2, 8, 4, 2, 2)
F32 = jnp.float32
BF16 = jnp.bfloat16
N = 512
TIMES = 128
HALF = 64
ROWS = 416


def place(time):
    rest, core = divmod(time, 2)
    rest, x = divmod(rest, 4)
    half, z = divmod(rest, 8)
    return half, z, x, core


def time_of(half, z, x, core):
    return ((half * 8 + z) * 4 + x) * 2 + core


def device(time, group):
    return time * 2 + group


def each():
    return ((time, group) for time in range(TIMES) for group in range(2))


def earlier(time, group, distance):
    target = (time - distance) % TIMES
    crossed = place(target)[0] != place(time)[0]
    return target, group ^ crossed


def ring_route(distance):
    return [(device(t, g), device(*earlier(t, g, distance))) for t, g in each()]


def round_x_holder(time, group):
    half, z, x, core = place(time)
    if x == 1:
        target, kept = earlier(time, group, 4)
        half, z, _, _ = place(target)
        return time_of(half, z, 2, core), kept
    return time_of(half, z, (x + 1) % 4, core), group


def round_x_first():
    return [(device(t, g), device(*round_x_holder(t, g))) for t, g in each()]


def round_x_second():
    return [(device(*round_x_holder(t, g)), device(*earlier(t, g, 4))) for t, g in each()]


def partner_group_route():
    return [(device(t, g), device(t, 1 - g)) for t, g in each()]


def other_core_route():
    return [(device(t, g), device(t ^ 1, g)) for t, g in each()]


def to_core(core):
    return [(device(t ^ 1, g), device(t, g)) for t, g in each() if t % 2 == core]


def of_core(route, core):
    return [(a, b) for a, b in route if (a // 2) % 2 == core]


def moved(array, route):
    return lax.ppermute(array, ALL, route)


TIME, GROUP, PAIRS, OTHER_PAIRS, DELTAS = 0, 1, 2, 8, 14
SMEM = pl.BlockSpec(memory_space=pltpu.SMEM)
VMEM = pl.BlockSpec(memory_space=pltpu.VMEM)
ANYWHERE = pl.BlockSpec(memory_space=pl.ANY)
HBM = pl.BlockSpec(memory_space=pltpu.HBM)


def fold(block):
    rows, columns = block.shape
    block = block.reshape(rows // 8, 8, columns).sum(0)
    return sum(block[:, i * 128 : (i + 1) * 128] for i in range(columns // 128))


def diagonal(block):
    rows = lax.broadcasted_iota(jnp.int32, block.shape, 0)
    columns = lax.broadcasted_iota(jnp.int32, block.shape, 1)
    return jnp.where(rows == columns, block, 0.0)


def product_terms(source, target, diff, total):
    direct = jnp.zeros((8, 128), F32)

    def dot(left, right):
        return jnp.dot(left, right, preferred_element_type=F32)

    for tile in range(2):
        columns = slice(tile * 256, (tile + 1) * 256)
        right_re = jnp.concatenate([piece[0, :, columns] for piece in target], axis=0)
        right_im = jnp.concatenate([piece[1, :, columns] for piece in target], axis=0)
        for half in range(2):
            rows = slice(half * 256, (half + 1) * 256)
            left_re, left_im = source[0, rows], source[1, rows]
            q_re = dot(left_re, right_re) - dot(left_im, right_im)
            q_im = dot(left_re, right_im) + dot(left_im, right_re)
            if half == tile:
                for k in range(2):
                    at = slice(k * 128, (k + 1) * 128)
                    direct = direct + fold(diagonal(q_re[at, at]))
            diff[rows, columns] = q_re - q_im
            total[rows, columns] = q_re + q_im
    box = jnp.zeros((8, 128), F32)
    for i in range(4):
        rows = slice(i * 128, (i + 1) * 128)
        for j in range(4):
            columns = slice(j * 128, (j + 1) * 128)
            box = box + fold(diff[rows, columns] * total[columns, rows].T)
    return direct, box


def add_terms(table, fields, result, sep, pieces, diff, total):
    time, group = table[TIME], table[GROUP]
    crossed = (time % HALF) + sep >= HALF
    shown = jnp.where(crossed, 1 - group, group)
    at = jnp.where(crossed, OTHER_PAIRS, PAIRS)
    row = sum(jnp.where(table[DELTAS + i] == sep - 1, i, 0) for i in range(4))
    lanes = lax.broadcasted_iota(jnp.int32, (1, 128), 1)
    for k in range(3):
        source = table[at + 2 * k]
        slot = source % 2 + jnp.where(source // 2 == group, 0, 2)
        momentum = table[at + 2 * k + 1] - 2 * shown

        target = [piece.at[momentum] for piece in pieces]
        direct, box = product_terms(fields.at[slot], target, diff.at[k % 2], total.at[k % 2])
        result = jnp.where(lanes == k * 4 + row, jnp.sum(direct), result)
        result = jnp.where(lanes == 12 + k * 4 + row, jnp.sum(box), result)
    return result


def first_body(table_in, own, other, near, out, fields, table, near_in, diff, total, sems):
    moves = [(table_in, table), (own, fields.at[0:2]), (other, fields.at[2:4]), (near, near_in)]
    copies = [pltpu.make_async_copy(a, b, sems.at[i]) for i, (a, b) in enumerate(moves)]
    for copy in copies[:3]:
        copy.start()
    copies[0].wait()
    core = table[TIME] % 2
    pl.when(core == 0)(copies[3].start)
    copies[1].wait()
    copies[2].wait()
    out[...] = jnp.zeros((1, 128), F32)

    @pl.when(core == 0)
    def _():
        copies[3].wait()
        out[...] = add_terms(table, fields, out[...], 1, [near_in], diff, total)


def by_core_body(table, fields, later0, later1, before, out, diff, total, *, seps):
    for core, later in enumerate((later0, later1)):

        @pl.when(table[TIME] % 2 == core)
        def _(core=core, later=later):
            out[...] = add_terms(
                table, fields, before[...], seps[core], [later], diff, total
            )


def late_body(table, fields, around, late, before, out, diff, total):
    out[...] = before[...]

    @pl.when(table[TIME] % 2 == 1)
    def _():
        out[...] = add_terms(table, fields, before[...], 3, [late, around], diff, total)


def four_body(table, fields, around, late, onward, rest, before, out, diff, total):
    for core, pieces in enumerate(([around, late], [onward, rest])):

        @pl.when(table[TIME] % 2 == core)
        def _(pieces=pieces):
            result = add_terms(table, fields, before[...], 4, pieces, diff, total)
            out[...] = jnp.broadcast_to(result[None], out.shape)


ROW = jax.ShapeDtypeStruct((1, 128), F32)
FIELDS = jax.ShapeDtypeStruct((4, 2, N, N), BF16)
PLANES = pltpu.VMEM((2, 2, N, N), BF16)
WORK = [pltpu.VMEM((2, N, N), F32), pltpu.VMEM((2, N, N), F32)]


def stage(body, operands, spaces, outs, scratch, products):
    call = pl.pallas_call(
        body,
        in_specs=spaces,
        out_specs=jax.tree.map(lambda _: VMEM, outs),
        out_shape=outs,
        scratch_shapes=scratch,
        compiler_params=pltpu.CompilerParams(vmem_limit_bytes=20 << 20),
        cost_estimate=pl.CostEstimate(
            flops=products * 8 * N**3, bytes_accessed=5 << 20, transcendentals=0
        ),
    )
    return call(*operands)


def zero_body(table, out):
    out[...] = jnp.zeros((1, 128), F32)


def mark_body(before, _, out):
    out[...] = before[...]


def finish_body(table, gathered, _, time_out, sum_out, time_row, sum_row, sems):
    time, group = table[TIME], table[GROUP]
    lanes = lax.broadcasted_iota(jnp.int32, (1, 128), 1)
    sep = jnp.zeros((1, 128), jnp.int32)
    for r in range(4):
        sep = jnp.where(lanes % 4 == r, table[DELTAS + r] + 1, sep)

    def value(at):
        crossed = (at % HALF) + sep >= HALF
        return jnp.where(crossed, gathered[2 * at + 1 - group], gathered[2 * at + group])

    def spread(row, out):
        for val in range(2):
            for k in range(3):
                at = val * 12 + k * 4
                shifted = pltpu.roll(row, 128 - at, 1) if at else row
                out[k, val : val + 1, :] = shifted[:, 0:4]

    spread(value(time), time_row.at[0])
    mine = pltpu.make_async_copy(time_row, time_out, sems.at[0])
    mine.start()
    total = jnp.zeros((1, 128), F32)
    for at in range(TIMES):
        if at % HALF < HALF - 4:
            total = total + gathered[2 * at + group]
        else:
            total = total + value(at)
    spread(total, sum_row)
    both = pltpu.make_async_copy(sum_row, sum_out, sems.at[1])
    both.start()
    mine.wait()
    both.wait()


def finished(table, gathered, ready):
    shapes = ((1, 3, 2, 4), (3, 2, 4))
    call = pl.pallas_call(
        finish_body,
        in_specs=[SMEM, VMEM, ANYWHERE],
        out_specs=(HBM, HBM),
        out_shape=tuple(jax.ShapeDtypeStruct(shape, F32) for shape in shapes),
        scratch_shapes=[pltpu.VMEM(shape, F32) for shape in shapes]
        + [pltpu.SemaphoreType.DMA((2,))],
        name="finish",
    )
    time_traces, summed_traces = call(table, gathered, ready)
    return time_traces.transpose(0, 2, 3, 1), summed_traces.transpose(1, 2, 0)


def per_device(fields, mom_pairs, deltas):
    own = fields[0]
    time = lax.axis_index(TM).astype(jnp.int32)
    group = lax.axis_index("mom").astype(jnp.int32)

    other_pairs = moved(mom_pairs, partner_group_route())
    other = moved(own, partner_group_route())
    two1 = moved(own, of_core(ring_route(2), 1))
    near = moved(own, other_core_route())
    half = N // 2
    around = jnp.where(time % 2 == 0, own[:, :, :half], near[:, :, half:])
    around = moved(around, round_x_first())
    table = jnp.concatenate(
        [jnp.stack([time, group]), mom_pairs.reshape(-1), other_pairs.reshape(-1), deltas]
    )
    zero = pl.pallas_call(zero_body, in_specs=[SMEM], out_specs=VMEM, out_shape=ROW, name="zero")
    mark = pl.pallas_call(
        mark_body, in_specs=[VMEM, VMEM], out_specs=VMEM, out_shape=ROW, name="mark"
    )
    ready = mark(zero(table), own)
    around = moved(around, round_x_second())
    two0 = moved(own, of_core(ring_route(2), 0))
    onward = moved(two1[:, :, :ROWS], of_core(ring_route(2), 1))
    swap1 = moved(two1, to_core(0))
    swap0 = moved(two0, to_core(1))
    rest = moved(own[:, :, ROWS:], of_core(round_x_first(), 1))
    rest = moved(rest, of_core(round_x_second(), 1))

    result, all_fields = stage(
        first_body,
        (table, own, other, near),
        [HBM, VMEM] + [ANYWHERE] * 2,
        (ROW, FIELDS),
        [pltpu.SMEM((18,), jnp.int32), PLANES] + WORK + [pltpu.SemaphoreType.DMA((4,))],
        3,
    )
    result = stage(
        functools.partial(by_core_body, seps=(2, 2)),
        (table, all_fields, two0, two1, result),
        [SMEM] + [VMEM] * 4,
        ROW,
        WORK,
        3,
    )
    late = moved(around, other_core_route())
    result = stage(
        functools.partial(by_core_body, seps=(3, 1)),
        (table, all_fields, swap1, swap0, result),
        [SMEM] + [VMEM] * 4,
        ROW,
        WORK,
        3,
    )
    result = stage(
        late_body, (table, all_fields, around, late, result), [SMEM] + [VMEM] * 4, ROW, WORK, 3
    )
    rows = stage(
        four_body,
        (table, all_fields, around, late, onward, rest, result),
        [SMEM] + [VMEM] * 6,
        jax.ShapeDtypeStruct((2 * TIMES, 1, 128), F32),
        WORK,
        3,
    )
    gathered = lax.all_to_all(rows, ALL, 0, 0, tiled=True)
    return finished(table, gathered, ready)


def solution(mesh):
    finer = Mesh(mesh.devices.reshape(SIZES), ALL)
    in_specs = (P(TM, "mom", None, None, None), P("mom", None), P())
    out_specs = (P(TM, None, None, "mom"), P(None, None, "mom"))
    return jax.shard_map(
        per_device, mesh=finer, in_specs=in_specs, out_specs=out_specs, check_vma=False
    )
```
